32 devices in a mesh: tm: 4 (over y, x), chan: 8 (over z, core).
Axes of the slice: x: 2, y: 2, z: 4, core: 2. Of those that a mesh axis runs over, the one named last changes fastest.
Arguments:
- observations: float32 [16, 64, 16384], P('chan', None, 'tm'), may hold values from -6 to 6
- transition: float32 [16, 128, 128], P('chan'), may hold values from -1 to 1, as said below
- obs_map: float32 [16, 64, 128], P('chan'), may hold values from -0.25 to 0.25
- measured_weighting: float32 [16, 64], P('chan'), may hold values from 0.05 to 0.5
- obs_precision: float32 [16, 64], P('chan'), may hold values from 0.3 to 9
- fading: float32 [16, 16384], P('chan', 'tm'), may hold values from 0.5 to 1
Outputs:
- states: float32 [16, 128, 16384], P('chan', None, 'tm')
- batch_nis: float32 [128], P('tm')
The draws below stay inside these ranges and needn't reach their ends.
Inputs may be any that keep to these rules, and one draw needn't show every extreme that they name: Each channel's transition is symmetric with all eigenvalues of magnitude below one.
All inputs are finite; a program needn't handle non-finite values.
Results may differ from the reference program's by a relative error of at most 0.0003.
Values sent between devices are 32-bit elements; how exact they have to be, the bound alone decides.
A program may use at most 64 MiB of HBM per device.

```python
import math
import jax
import jax.numpy as jnp
from jax import lax

STATE = 128
OBS = 64
MB_FRAMES = 128
PROBE_COUNT = 16
TIMESTEP_COUNT = 16384
MICRO_BATCHES = 128


def draw_transition(key, part):
    first, latter_portion, third = jax.random.split(key, 3)
    upper = math.log(0.05)
    rates = jnp.exp(jax.random.uniform(first, (PROBE_COUNT, STATE), jnp.float32, math.log(0.0001), upper))
    signs = jnp.where(jax.random.randint(latter_portion, (PROBE_COUNT, STATE), 0, 2) == 0, -1.0, 1.0)
    eigen = signs * jnp.exp(-rates)
    basis, unused = jnp.linalg.qr(jax.random.normal(third, (PROBE_COUNT, STATE, STATE), jnp.float32))
    return jnp.einsum('cst,ct,cut->csu', basis, eigen, basis).astype(jnp.float32)


def draw_obs_precision(key, part):
    ramp = 1.0 + 2.0 * jnp.arange(PROBE_COUNT, dtype=jnp.float32) / max(PROBE_COUNT - 1, 1)
    spread = jax.random.uniform(key, (PROBE_COUNT, OBS), jnp.float32, 0.5, 1.5)
    return (spread * ramp[:, None]).astype(jnp.float32)


def draw_fading(key, part):
    first, latter_portion, third = jax.random.split(key, 3)
    lower = 0.9995
    standard_branch = jax.random.uniform(first, (PROBE_COUNT, TIMESTEP_COUNT), jnp.float32, lower, 1.0)
    clustered_blocks = jax.random.bernoulli(latter_portion, 3.0 / TIMESTEP_COUNT, (PROBE_COUNT, TIMESTEP_COUNT))
    discarded_entries = jax.random.uniform(third, (PROBE_COUNT, TIMESTEP_COUNT), jnp.float32, 0.5, 0.8)
    return jnp.where(clustered_blocks, discarded_entries, standard_branch).astype(jnp.float32)


def levels(key, shape, pieces, least, largest):
    level, own = 1.0, jax.random.fold_in(key, 6)
    for position, parts in pieces:
        draws = jnp.exp(jax.random.uniform(jax.random.fold_in(own, position), (parts,), jnp.float32, least / len(pieces), largest / len(pieces)))
        level = level * jnp.repeat(draws, shape[position] // parts).reshape([-1 if axis == position else 1 for axis in range(len(shape))])
    return level


def bell_draw(rng, dims, scale, most, cuts=(), kind=jnp.bfloat16):
    values = jax.random.normal(rng, dims, jnp.float32) * scale
    if len(cuts) > 0:
        values = levels(rng, dims, cuts, -0.22, 0.18) * values
    return jnp.clip(values, min=-most, max=most).astype(kind)


def setup_inputs(seed: int = 0) -> dict:
    splits = jax.random.split(jax.random.key(seed), 7)
    return {
        "observations": bell_draw(splits[0], (PROBE_COUNT, OBS, TIMESTEP_COUNT), 1.0, 6.0, ((0, 8), (2, 4)), jnp.float32),
        "transition": draw_transition(jax.random.fold_in(splits[6], 71), 0),
        "obs_map": bell_draw(splits[2], (PROBE_COUNT, OBS, STATE), (4 * STATE) ** -0.5, 0.25, ((0, 8),), jnp.float32),
        "measured_weighting": jnp.clip(jnp.exp(math.log(0.5) - 2.3025851 * jax.random.uniform(splits[3], (PROBE_COUNT, OBS), jnp.float32) ** levels(splits[3], (PROBE_COUNT, OBS), ((0, 8),), -0.2, 0.2)), 0.05, 0.5),
        "obs_precision": draw_obs_precision(jax.random.fold_in(splits[6], 71), 0),
        "fading": draw_fading(jax.random.fold_in(splits[6], 71), 0),
    }


def filter_block(argument_list):
    transition, obs_map, measured_weighting, obs_precision, observations, fading = argument_list
    highest = lax.Precision.HIGHEST
    gain = jnp.swapaxes(obs_map, 1, 2) * measured_weighting[:, None, :]

    def advance(carried, inputs):
        frame_obs, frame_fading = inputs
        predicted = frame_fading[:, None] * jnp.einsum('bst,bt->bs', transition, carried, precision=highest)
        innovation = frame_obs - jnp.einsum('bos,bs->bo', obs_map, predicted, precision=highest)
        updated = predicted + jnp.einsum('bso,bo->bs', gain, innovation, precision=highest)
        frame_nis = jnp.sum(obs_precision * innovation * innovation)
        return (updated, (updated, frame_nis))
    initial = jnp.zeros((transition.shape[0], transition.shape[1]), jnp.float32)
    inputs = (jnp.moveaxis(observations, 2, 0), jnp.transpose(fading))
    unused, (history, frame_norms) = lax.scan(advance, initial, inputs)
    return (jnp.moveaxis(history, 0, 2), frame_norms)

def reference(observations, transition, obs_map, measured_weighting, obs_precision, fading):
    block_size = math.gcd(PROBE_COUNT, 64)
    blocks = PROBE_COUNT // block_size

    def split_blocks(array):
        return array.reshape((blocks, block_size) + array.shape[1:])
    argument_list = (split_blocks(transition), split_blocks(obs_map), split_blocks(measured_weighting), split_blocks(obs_precision), split_blocks(observations), split_blocks(fading))
    history, frame_norms = lax.map(filter_block, argument_list)
    states = history.reshape(PROBE_COUNT, STATE, TIMESTEP_COUNT)
    totals = jnp.sum(frame_norms, axis=0)
    batch_nis = jnp.sum(totals.reshape(MICRO_BATCHES, MB_FRAMES), axis=1) / (PROBE_COUNT * MB_FRAMES * OBS)
    return (states, batch_nis)
```

```python
import functools

import jax
import jax.numpy as jnp
from jax import lax
from jax.experimental import pallas as pl
from jax.experimental.pallas import tpu as pltpu
from jax.sharding import PartitionSpec as P

MB_FRAMES = 128
CHUNK = 16
HIGHEST = lax.Precision.HIGHEST
F32 = jnp.float32
BF16 = jnp.bfloat16


def dot(a, b, dims=((1,), (0,)), precision=HIGHEST):
    return lax.dot_general(a, b, (dims, ((), ())), precision=precision, preferred_element_type=F32)


def halves(x):
    high = x.astype(BF16)
    low = (x - high.astype(F32)).astype(BF16)
    return high, low


def rows_split(x):
    return jnp.concatenate(halves(x), axis=1)


def pack(weight):
    high, low = halves(weight)
    top = jnp.concatenate([high, low], axis=1)
    return jnp.concatenate([top, top], axis=0)


def fast(split, packed):
    both = dot(split, packed, precision=None)
    half = both.shape[1] // 2
    return both[:, :half] + both[:, half:]


def shifted(x, reach, fill, row):
    return jnp.where(row >= reach, pltpu.roll(x, reach, 0), fill)


def kernel(
    tm, chan, y_hbm, trans_ref, map_ref, weight_ref, prec_ref, fade_ref, states_hbm, nis_ref,
    y_ref, yt_ref, ft_ref, xt_ref, out_ref, end_src, end_got, nis_src, nis_got,
    in_sem, out_sem, end_send, end_recv, nis_send, nis_recv,
):
    channels, obs, frames = y_ref.shape
    state = trans_ref.shape[1]
    length = CHUNK
    count = frames // length
    my_tm, my_chan = lax.axis_index("tm"), lax.axis_index("chan")

    def peer(axis, size, mine, offset):
        return {axis: lax.rem(mine + offset, size)}

    peers = [peer("tm", tm, my_tm, d) for d in range(1, tm)]
    peers += [peer("chan", chan, my_chan, d) for d in range(1, chan)]
    barrier = pltpu.get_barrier_semaphore()
    for target in peers:
        pl.semaphore_signal(barrier, inc=1, device_id=target, device_id_type=pl.DeviceIdType.MESH)
    load = pltpu.make_async_copy(y_hbm, y_ref, in_sem)
    load.start()

    each = range(channels)
    lanes = channels * obs
    eye = lax.broadcasted_iota(jnp.int32, (obs, obs), 0) == lax.broadcasted_iota(jnp.int32, (obs, obs), 1)
    owner = lax.broadcasted_iota(jnp.int32, (1, lanes), 1) // obs

    fade = fade_ref[...]
    ft_ref[...] = jnp.transpose(jnp.concatenate([fade] * (8 // channels), axis=0))

    def fade_at(step):
        return ft_ref[pl.ds(step, count, stride=length), :]

    def fade_lanes(columns):
        out = jnp.broadcast_to(columns[:, 0:1], (count, lanes))
        for c in each[1:]:
            out = jnp.where(owner == c, columns[:, c : c + 1], out)
        return out

    weighted, closed, map_trans = [], [], []
    for c in each:
        column = jnp.sum(jnp.where(eye, weight_ref[c : c + 1, :], 0.0), axis=1, keepdims=True)
        observe = map_ref[c]
        weighted.append(observe * column)
        moved = dot(observe, trans_ref[c])
        map_trans.append(jnp.transpose(moved))
        closed.append(jnp.transpose(trans_ref[c]) - dot(moved, weighted[c], ((0,), (0,))))

    stacks, power = list(weighted), list(closed)
    reach = 1
    while reach < length:
        for c in each:
            stacks[c] = jnp.concatenate([stacks[c], dot(stacks[c], power[c])], axis=0)
            power[c] = dot(power[c], power[c])
        reach *= 2

    def spread(blocks):
        rows = []
        for c in each:
            parts = [blocks[c] if d == c else jnp.zeros_like(blocks[c]) for d in each]
            rows.append(jnp.concatenate(parts, axis=1))
        return jnp.concatenate(rows, axis=0)

    def inject_weight(blocks):
        high, low = halves(spread(blocks))
        return jnp.concatenate([high, high, low], axis=0)

    def inject(values, weight):
        high, low = halves(values)
        return dot(jnp.concatenate([high, low, high], axis=1), weight, precision=None)

    load.wait()
    block = min(frames, 512)
    for start in range(0, frames, block):
        piece = y_ref[:, :, start : start + block].reshape(lanes, block)
        yt_ref[start : start + block, :] = jnp.transpose(piece)

    def obs_at(step):
        return yt_ref[pl.ds(step, count, stride=length), :]

    ends = jnp.zeros((count, channels * state), F32)
    decay = jnp.ones((count, lanes), F32)
    for step in reversed(range(length)):
        age = length - 1 - step
        blocks = [stacks[c][age * obs : (age + 1) * obs] for c in each]
        ends = ends + inject(obs_at(step) * decay, inject_weight(blocks))
        decay = decay * fade_lanes(fade_at(step))

    row = lax.broadcasted_iota(jnp.int32, (count, state), 0)
    sums = [ends[:, c * state : (c + 1) * state] for c in each]
    factors = [jnp.broadcast_to(decay[:, c * obs : c * obs + 1], (count, state)) for c in each]
    packed = []
    reach = 1
    while reach < count:
        packed.append([pack(power[c]) for c in each])
        for c in each:
            before = rows_split(shifted(sums[c], reach, 0.0, row))
            sums[c] = sums[c] + factors[c] * fast(before, packed[-1][c])
            factors[c] = factors[c] * shifted(factors[c], reach, 1.0, row)
            power[c] = dot(power[c], power[c])
        reach *= 2

    last = [part[c][count - 1 : count, :] for part in (sums, factors) for c in each]
    end_src[...] = jnp.concatenate(last + [jnp.zeros((8 - len(last), state), F32)], axis=0)
    pl.semaphore_wait(barrier, len(peers))
    sends = []
    for d in range(1, tm):
        copy = pltpu.make_async_remote_copy(
            src_ref=end_src, dst_ref=end_got.at[d - 1], send_sem=end_send.at[d - 1],
            recv_sem=end_recv.at[d - 1], device_id=peers[d - 1], device_id_type=pl.DeviceIdType.MESH,
        )
        copy.start()
        sends.append(copy)

    sums = [shifted(sums[c], 1, 0.0, row) for c in each]
    factors = [shifted(factors[c], 1, 1.0, row) for c in each]
    step_weight = [pack(closed[c]) for c in each]
    pred_weight = []
    for c in each:
        parts = [map_trans[c] if d == c else jnp.zeros_like(map_trans[c]) for d in each]
        pred_weight.append(pack(jnp.concatenate(parts, axis=1)))
    now_weight = inject_weight(weighted)
    section = [pack(power[c]) for c in each]

    for copy in sends:
        copy.wait()

    enter = [jnp.zeros((8, state), F32) for c in each]
    for j in range(tm - 1):
        slot = jnp.maximum(lax.rem(my_tm - j + tm, tm) - 1, 0)
        got = end_got[slot]
        for c in each:
            value = jnp.broadcast_to(got[c : c + 1, :], (8, state))
            if j > 0:
                value = value + got[channels + c : channels + c + 1, :] * fast(
                    rows_split(enter[c]), section[c]
                )
            enter[c] = jnp.where(j < my_tm, value, enter[c])

    x = []
    small = lax.broadcasted_iota(jnp.int32, (8, state), 0)
    for c in each:
        carried = enter[c]
        for level, weights in enumerate(packed):
            further = fast(rows_split(carried), weights[c])
            size = 1 << level
            if size < 8:
                carried = jnp.where(small < size, carried, pltpu.roll(further, size, 0))
            else:
                carried = jnp.concatenate([carried, further], axis=0)
        x.append(sums[c] + factors[c] * carried[:count])

    prec = jnp.concatenate([prec_ref[c : c + 1, :] for c in each], axis=1)
    norms = jnp.zeros((count, lanes), F32)
    for step in range(length):
        observed = obs_at(step)
        columns = fade_at(step)
        added = inject(observed, now_weight)
        innovation = observed
        for c in each:
            split = rows_split(x[c])
            wide = jnp.broadcast_to(columns[:, c : c + 1], (count, state))
            innovation = innovation - columns[:, c : c + 1] * fast(split, pred_weight[c])
            x[c] = wide * fast(split, step_weight[c]) + added[:, c * state : (c + 1) * state]
            xt_ref[c, pl.ds(step, count, stride=length), :] = x[c]
        norms = norms + prec * innovation * innovation

    batches = nis_ref.shape[1]
    per_batch = jnp.sum(norms.reshape(batches, count // batches, lanes), axis=1)
    nis_src[...] = dot(jnp.ones((8, lanes), F32), per_batch, ((1,), (1,)))
    sends = []
    for d in range(1, chan):
        copy = pltpu.make_async_remote_copy(
            src_ref=nis_src, dst_ref=nis_got.at[d - 1], send_sem=nis_send.at[d - 1],
            recv_sem=nis_recv.at[d - 1], device_id=peers[tm - 1 + d - 1],
            device_id_type=pl.DeviceIdType.MESH,
        )
        copy.start()
        sends.append(copy)

    stores = []
    for c in each:
        for index, start in enumerate(range(0, frames, block)):
            out_ref[c, :, start : start + block] = jnp.transpose(xt_ref[c, start : start + block, :])
            store = pltpu.make_async_copy(
                out_ref.at[c, :, pl.ds(start, block)],
                states_hbm.at[c, :, pl.ds(start, block)],
                out_sem.at[c, index],
            )
            store.start()
            stores.append(store)

    for copy in sends:
        copy.wait()
    total = nis_src[0:1, :]
    for d in range(1, chan):
        total = total + nis_got[d - 1, 0:1, :]
    nis_ref[...] = total / (channels * chan * MB_FRAMES * obs)
    for store in stores:
        store.wait()


def per_device(tm, chan, observations, transition, obs_map, measured_weighting, obs_precision, fading):
    channels, obs, frames = observations.shape
    state = transition.shape[1]
    batches = frames // MB_FRAMES
    lanes = channels * obs
    vmem = pl.BlockSpec(memory_space=pltpu.VMEM)
    hbm = pl.BlockSpec(memory_space=pl.ANY)
    dma = pltpu.SemaphoreType.DMA
    blocks = frames // min(frames, 512)
    states, nis = pl.pallas_call(
        functools.partial(kernel, tm, chan),
        out_shape=(
            jax.ShapeDtypeStruct((channels, state, frames), F32),
            jax.ShapeDtypeStruct((1, batches), F32),
        ),
        in_specs=[hbm] + [vmem] * 5,
        out_specs=(hbm, vmem),
        scratch_shapes=[
            pltpu.VMEM((channels, obs, frames), F32),
            pltpu.VMEM((frames, lanes), F32),
            pltpu.VMEM((frames, 8), F32),
            pltpu.VMEM((channels, frames, state), F32),
            pltpu.VMEM((channels, state, frames), F32),
            pltpu.VMEM((8, state), F32),
            pltpu.VMEM((max(tm - 1, 1), 8, state), F32),
            pltpu.VMEM((8, batches), F32),
            pltpu.VMEM((max(chan - 1, 1), 8, batches), F32),
            dma(()),
            dma((channels, blocks)),
            dma((max(tm - 1, 1),)),
            dma((max(tm - 1, 1),)),
            dma((max(chan - 1, 1),)),
            dma((max(chan - 1, 1),)),
        ],
        compiler_params=pltpu.CompilerParams(
            collective_id=0, has_side_effects=True, vmem_limit_bytes=56 * 1024 * 1024
        ),
        name="filter",
    )(observations, transition, obs_map, measured_weighting, obs_precision, fading)
    return states, nis.reshape(batches)


def solution(mesh):
    in_specs = (
        P("chan", None, "tm"),
        P("chan", None, None),
        P("chan", None, None),
        P("chan", None),
        P("chan", None),
        P("chan", "tm"),
    )
    out_specs = (P("chan", None, "tm"), P("tm"))
    body = functools.partial(per_device, mesh.shape["tm"], mesh.shape["chan"])
    return jax.shard_map(body, mesh=mesh, in_specs=in_specs, out_specs=out_specs, check_vma=False)
```

```python
import functools

import jax
import jax.numpy as jnp
from jax import lax
from jax.experimental import pallas as pl
from jax.experimental.pallas import tpu as pltpu
from jax.sharding import PartitionSpec as P

MB_FRAMES = 128
LANES = 128
GROUP = 8
CHUNK = LANES // GROUP
HIGHEST = lax.Precision.HIGHEST
F32 = jnp.float32
BF16 = jnp.bfloat16


def dot(a, b, dims=((1,), (0,)), precision=HIGHEST):
    return lax.dot_general(a, b, (dims, ((), ())), precision=precision, preferred_element_type=F32)


def halves(x):
    high = x.astype(BF16)
    low = (x - high.astype(F32)).astype(BF16)
    return high, low


def rows_split(x):
    return jnp.concatenate(halves(x), axis=1)


def pack(weight):
    high, low = halves(weight)
    top = jnp.concatenate([high, low], axis=1)
    return jnp.concatenate([top, top], axis=0)


def fast(split, packed):
    both = dot(split, packed, precision=None)
    half = both.shape[1] // 2
    return both[:, :half] + both[:, half:]


def regroup(x, groups):
    place = lax.broadcasted_iota(jnp.int32, x.shape, 1)
    source = (place % groups) * (LANES // groups) + place // groups
    return jnp.take_along_axis(x, source, axis=1, mode="promise_in_bounds")


def shifted(x, reach, fill, row):
    return jnp.where(row >= reach, pltpu.roll(x, reach, 0), fill)


def kernel(
    tm, chan, y_hbm, trans_ref, map_ref, weight_ref, prec_ref, fade_ref, states_hbm, nis_ref,
    y_ref, yt_ref, ft_ref, xt_ref, end_src, end_got, nis_src, nis_got,
    in_sem, out_sem, end_send, end_recv, nis_send, nis_recv,
):
    channels, obs, frames = y_ref.shape
    state = trans_ref.shape[1]
    length = CHUNK
    count = frames // length
    my_tm, my_chan = lax.axis_index("tm"), lax.axis_index("chan")

    def peer(axis, size, mine, offset):
        return {axis: lax.rem(mine + offset, size)}

    peers = [peer("tm", tm, my_tm, d) for d in range(1, tm)]
    peers += [peer("chan", chan, my_chan, d) for d in range(1, chan)]
    barrier = pltpu.get_barrier_semaphore()
    for target in peers:
        pl.semaphore_signal(barrier, inc=1, device_id=target, device_id_type=pl.DeviceIdType.MESH)
    load = pltpu.make_async_copy(y_hbm, y_ref, in_sem)
    load.start()

    each = range(channels)
    lanes = channels * obs
    eye = lax.broadcasted_iota(jnp.int32, (obs, obs), 0) == lax.broadcasted_iota(jnp.int32, (obs, obs), 1)
    owner = lax.broadcasted_iota(jnp.int32, (1, lanes), 1) // obs

    fade = jnp.concatenate([fade_ref[...]] * (8 // channels), axis=0)
    for b in range(frames // LANES):
        piece = regroup(fade[:, b * LANES : (b + 1) * LANES], GROUP)
        ft_ref[b] = jnp.transpose(piece).reshape(length, GROUP, 8)

    def fade_at(step):
        return ft_ref[:, step].reshape(count, 8)

    def fade_lanes(columns):
        out = jnp.broadcast_to(columns[:, 0:1], (count, lanes))
        for c in each[1:]:
            out = jnp.where(owner == c, columns[:, c : c + 1], out)
        return out

    weighted, closed, map_trans = [], [], []
    for c in each:
        column = jnp.sum(jnp.where(eye, weight_ref[c : c + 1, :], 0.0), axis=1, keepdims=True)
        observe = map_ref[c]
        weighted.append(observe * column)
        moved = dot(observe, trans_ref[c])
        map_trans.append(jnp.transpose(moved))
        closed.append(jnp.transpose(trans_ref[c]) - dot(moved, weighted[c], ((0,), (0,))))

    load.wait()
    blocks_all = frames // LANES

    def turn(first, last):
        for b in range(first, last):
            piece = y_ref[:, :, b * LANES : (b + 1) * LANES].reshape(lanes, LANES)
            yt_ref[b] = jnp.transpose(regroup(piece, GROUP)).reshape(length, GROUP, lanes)

    stacks, power = list(weighted), list(closed)
    rounds = length.bit_length() - 1
    for level in range(rounds):
        turn(level * blocks_all // rounds, (level + 1) * blocks_all // rounds)
        for c in each:
            older = fast(rows_split(stacks[c]), pack(power[c]))
            stacks[c] = jnp.concatenate([stacks[c], older], axis=0)
            power[c] = dot(power[c], power[c])

    def spread(blocks):
        rows = []
        for c in each:
            parts = [blocks[c] if d == c else jnp.zeros_like(blocks[c]) for d in each]
            rows.append(jnp.concatenate(parts, axis=1))
        return jnp.concatenate(rows, axis=0)

    def inject_weight(blocks):
        high, low = halves(spread(blocks))
        return jnp.concatenate([high, high, low], axis=0)

    def inject(values, weight):
        high, low = halves(values)
        return dot(jnp.concatenate([high, low, high], axis=1), weight, precision=None)

    def obs_at(step):
        return yt_ref[:, step].reshape(count, lanes)

    ends = jnp.zeros((count, channels * state), F32)
    decay = jnp.ones((count, lanes), F32)
    packed = []
    levels = count.bit_length() - 1
    every = max(length // levels, 1)
    for step in reversed(range(length)):
        age = length - 1 - step
        blocks = [stacks[c][age * obs : (age + 1) * obs] for c in each]
        ends = ends + inject(obs_at(step) * decay, inject_weight(blocks))
        decay = decay * fade_lanes(fade_at(step))
        if len(packed) < levels and age % every == 0:
            packed.append([pack(power[c]) for c in each])
            power = [dot(power[c], power[c]) for c in each]

    row = lax.broadcasted_iota(jnp.int32, (count, state), 0)
    sums = [ends[:, c * state : (c + 1) * state] for c in each]
    factors = [jnp.broadcast_to(decay[:, c * obs : c * obs + 1], (count, state)) for c in each]
    while len(packed) < levels:
        packed.append([pack(power[c]) for c in each])
        power = [dot(power[c], power[c]) for c in each]
    for level in range(levels):
        reach = 1 << level
        for c in each:
            if reach < GROUP:
                before = rows_split(shifted(sums[c], reach, 0.0, row))
                sums[c] = sums[c] + factors[c] * fast(before, packed[level][c])
                factors[c] = factors[c] * shifted(factors[c], reach, 1.0, row)
            else:
                rest = count - reach
                moved = factors[c][reach:] * fast(rows_split(sums[c][:rest]), packed[level][c])
                sums[c] = jnp.concatenate([sums[c][:reach], sums[c][reach:] + moved], axis=0)
                joined = factors[c][reach:] * factors[c][:rest]
                factors[c] = jnp.concatenate([factors[c][:reach], joined], axis=0)

    last = [part[c][count - 1 : count, :] for part in (sums, factors) for c in each]
    end_src[...] = jnp.concatenate(last + [jnp.zeros((8 - len(last), state), F32)], axis=0)
    pl.semaphore_wait(barrier, len(peers))
    sends = []
    for d in range(1, tm):
        copy = pltpu.make_async_remote_copy(
            src_ref=end_src, dst_ref=end_got.at[d - 1], send_sem=end_send.at[d - 1],
            recv_sem=end_recv.at[d - 1], device_id=peers[d - 1], device_id_type=pl.DeviceIdType.MESH,
        )
        copy.start()
        sends.append(copy)

    sums = [shifted(sums[c], 1, 0.0, row) for c in each]
    factors = [shifted(factors[c], 1, 1.0, row) for c in each]
    step_weight = [pack(closed[c]) for c in each]
    pred_weight = []
    for c in each:
        parts = [map_trans[c] if d == c else jnp.zeros_like(map_trans[c]) for d in each]
        pred_weight.append(pack(jnp.concatenate(parts, axis=1)))
    now_weight = inject_weight(weighted)
    section = [pack(power[c]) for c in each]

    for copy in sends:
        copy.wait()

    enter = [jnp.zeros((8, state), F32) for c in each]
    for j in range(tm - 1):
        slot = jnp.maximum(lax.rem(my_tm - j + tm, tm) - 1, 0)
        got = end_got[slot]
        for c in each:
            value = jnp.broadcast_to(got[c : c + 1, :], (8, state))
            if j > 0:
                value = value + got[channels + c : channels + c + 1, :] * fast(
                    rows_split(enter[c]), section[c]
                )
            enter[c] = jnp.where(j < my_tm, value, enter[c])

    x = []
    small = lax.broadcasted_iota(jnp.int32, (8, state), 0)
    for c in each:
        carried = enter[c]
        for level, weights in enumerate(packed):
            further = fast(rows_split(carried), weights[c])
            size = 1 << level
            if size < 8:
                carried = jnp.where(small < size, carried, pltpu.roll(further, size, 0))
            else:
                carried = jnp.concatenate([carried, further], axis=0)
        x.append(sums[c] + factors[c] * carried[:count])

    prec = jnp.concatenate([prec_ref[c : c + 1, :] for c in each], axis=1)
    norms = jnp.zeros((count, lanes), F32)
    stores = []
    for step in range(length):
        observed = obs_at(step)
        columns = fade_at(step)
        added = inject(observed, now_weight)
        innovation = observed
        for c in each:
            split = rows_split(x[c])
            wide = jnp.broadcast_to(columns[:, c : c + 1], (count, state))
            innovation = innovation - columns[:, c : c + 1] * fast(split, pred_weight[c])
            x[c] = wide * fast(split, step_weight[c]) + added[:, c * state : (c + 1) * state]
            xt_ref[c, :, step] = x[c].reshape(blocks_all, GROUP, state)
            store = pltpu.make_async_copy(
                xt_ref.at[c, :, step], states_hbm.at[c, :, step], out_sem.at[c, step]
            )
            store.start()
            stores.append(store)
        norms = norms + prec * innovation * innovation

    batches = nis_ref.shape[1]
    per_batch = jnp.sum(norms.reshape(batches, count // batches, lanes), axis=1)
    nis_src[...] = dot(jnp.ones((8, lanes), F32), per_batch, ((1,), (1,)))
    sends = []
    for d in range(1, chan):
        copy = pltpu.make_async_remote_copy(
            src_ref=nis_src, dst_ref=nis_got.at[d - 1], send_sem=nis_send.at[d - 1],
            recv_sem=nis_recv.at[d - 1], device_id=peers[tm - 1 + d - 1],
            device_id_type=pl.DeviceIdType.MESH,
        )
        copy.start()
        sends.append(copy)

    for copy in sends:
        copy.wait()
    total = nis_src[0:1, :]
    for d in range(1, chan):
        total = total + nis_got[d - 1, 0:1, :]
    nis_ref[...] = total / (channels * chan * MB_FRAMES * obs)
    for store in stores:
        store.wait()


def turn_states(x_ref, out_ref):
    for start in range(0, x_ref.shape[1], LANES):
        piece = jnp.transpose(x_ref[0, start : start + LANES, :])
        out_ref[0, :, start : start + LANES] = regroup(piece, CHUNK)


def per_device(tm, chan, observations, transition, obs_map, measured_weighting, obs_precision, fading):
    channels, obs, frames = observations.shape
    state = transition.shape[1]
    batches = frames // MB_FRAMES
    lanes = channels * obs
    vmem = pl.BlockSpec(memory_space=pltpu.VMEM)
    hbm = pl.BlockSpec(memory_space=pl.ANY)
    dma = pltpu.SemaphoreType.DMA
    grouped = (channels, frames // LANES, CHUNK, GROUP, state)
    turned, nis = pl.pallas_call(
        functools.partial(kernel, tm, chan),
        out_shape=(
            jax.ShapeDtypeStruct(grouped, F32),
            jax.ShapeDtypeStruct((1, batches), F32),
        ),
        in_specs=[hbm] + [vmem] * 5,
        out_specs=(hbm, vmem),
        scratch_shapes=[
            pltpu.VMEM((channels, obs, frames), F32),
            pltpu.VMEM((frames // LANES, CHUNK, GROUP, lanes), F32),
            pltpu.VMEM((frames // LANES, CHUNK, GROUP, 8), F32),
            pltpu.VMEM(grouped, F32),
            pltpu.VMEM((8, state), F32),
            pltpu.VMEM((max(tm - 1, 1), 8, state), F32),
            pltpu.VMEM((8, batches), F32),
            pltpu.VMEM((max(chan - 1, 1), 8, batches), F32),
            dma(()),
            dma((channels, CHUNK)),
            dma((max(tm - 1, 1),)),
            dma((max(tm - 1, 1),)),
            dma((max(chan - 1, 1),)),
            dma((max(chan - 1, 1),)),
        ],
        compiler_params=pltpu.CompilerParams(
            collective_id=0, has_side_effects=True, vmem_limit_bytes=56 * 1024 * 1024
        ),
        name="filter",
    )(observations, transition, obs_map, measured_weighting, obs_precision, fading)
    block = min(frames, 1024)
    states = pl.pallas_call(
        turn_states,
        grid=(channels, frames // block),
        out_shape=jax.ShapeDtypeStruct((channels, state, frames), F32),
        in_specs=[pl.BlockSpec((1, block, state), lambda c, b: (c, b, 0))],
        out_specs=pl.BlockSpec((1, state, block), lambda c, b: (c, 0, b)),
        name="turn",
    )(turned.reshape(channels, frames, state))
    return states, nis.reshape(batches)


def solution(mesh):
    in_specs = (
        P("chan", None, "tm"),
        P("chan", None, None),
        P("chan", None, None),
        P("chan", None),
        P("chan", None),
        P("chan", "tm"),
    )
    out_specs = (P("chan", None, "tm"), P("tm"))
    body = functools.partial(per_device, mesh.shape["tm"], mesh.shape["chan"])
    return jax.shard_map(body, mesh=mesh, in_specs=in_specs, out_specs=out_specs, check_vma=False)
```

```python
import functools

import jax
import jax.numpy as jnp
from jax import lax
from jax.experimental import pallas as pl
from jax.experimental.pallas import tpu as pltpu
from jax.sharding import PartitionSpec as P

MB_FRAMES = 128
LANES = 128
GROUP = 8
PARTS = 1
SPANS = 2
CHUNK = LANES // GROUP
HIGHEST = lax.Precision.HIGHEST
F32 = jnp.float32
BF16 = jnp.bfloat16


def dot(a, b, dims=((1,), (0,)), precision=HIGHEST):
    return lax.dot_general(a, b, (dims, ((), ())), precision=precision, preferred_element_type=F32)


def halves(x):
    high = x.astype(BF16)
    low = (x - high.astype(F32)).astype(BF16)
    return high, low


def thirds(x):
    high = x.astype(BF16)
    rest = x - high.astype(F32)
    mid = rest.astype(BF16)
    return high, mid, (rest - mid.astype(F32)).astype(BF16)


def exact(a, b):
    a_high, a_mid, a_low = thirds(a)
    b_high, b_mid, b_low = thirds(b)
    top = jnp.concatenate([b_high, b_mid], axis=1)
    wide = dot(
        jnp.concatenate([a_high, a_mid], axis=1),
        jnp.concatenate([top, top], axis=0),
        precision=None,
    )
    tail = dot(
        jnp.concatenate([a_high, a_low], axis=1),
        jnp.concatenate([b_low, b_high], axis=0),
        precision=None,
    )
    half = b.shape[1]
    return wide[:, :half] + (wide[:, half:] + tail)


def rows_split(x):
    return jnp.concatenate(halves(x), axis=1)


def pack(weight):
    high, low = halves(weight)
    top = jnp.concatenate([high, low], axis=1)
    return jnp.concatenate([top, top], axis=0)


def fast(split, packed):
    both = dot(split, packed, precision=None)
    half = both.shape[1] // 2
    return both[:, :half] + both[:, half:]


def regroup(x, groups):
    place = lax.broadcasted_iota(jnp.int32, x.shape, 1)
    source = (place % groups) * (LANES // groups) + place // groups
    return jnp.take_along_axis(x, source, axis=1, mode="promise_in_bounds")


def turn_fading(fade):
    frames = fade.shape[1]
    rows = [fade[:, b : b + LANES] for b in range(0, frames, LANES)]
    filled = sum(part.shape[0] for part in rows)
    rows.append(jnp.zeros((-filled % LANES, LANES), F32))
    return jnp.transpose(regroup(jnp.concatenate(rows, axis=0), GROUP))


def fade_wide(ft_ref, step, c, channels, span):
    here = ft_ref[step * GROUP : (step + 1) * GROUP, :]
    parts = []
    for b in range(span.start, span.stop):
        lane = b * channels + c
        parts.append(jnp.broadcast_to(here[:, lane : lane + 1], (GROUP, LANES)))
    return jnp.concatenate(parts, axis=0)


def inject(values, weight):
    high, low = halves(values)
    return dot(jnp.concatenate([high, low, high], axis=1), weight, precision=None)


def shifted(x, reach, fill, row):
    return jnp.where(row >= reach, pltpu.roll(x, reach, 0), fill)


def greet(axis, size, mine):
    peers = [{axis: lax.rem(mine + d, size)} for d in range(1, size)]
    barrier = pltpu.get_barrier_semaphore()
    for target in peers:
        pl.semaphore_signal(barrier, inc=1, device_id=target, device_id_type=pl.DeviceIdType.MESH)
    return barrier, peers


def swap(src, got, send_sem, recv_sem, peers):
    sends = []
    for d, target in enumerate(peers):
        copy = pltpu.make_async_remote_copy(
            src_ref=src, dst_ref=got.at[d], send_sem=send_sem.at[d], recv_sem=recv_sem.at[d],
            device_id=target, device_id_type=pl.DeviceIdType.MESH,
        )
        copy.start()
        sends.append(copy)
    return sends


def enter_kernel(
    tm, y_hbm, trans_ref, map_ref, weight_ref, fade_ref,
    yt_hbm, ft_ref, x_ref, step_ref, pred_ref, now_ref,
    y_ref, yt_ref, end_src, end_got, in_sem, yt_sem, end_send, end_recv,
):
    channels, obs, frames = y_ref.shape
    state = trans_ref.shape[1]
    length = CHUNK
    count = frames // length
    my_tm = lax.axis_index("tm")
    barrier, peers = greet("tm", tm, my_tm)
    load = pltpu.make_async_copy(y_hbm, y_ref, in_sem)
    load.start()

    each = range(channels)
    lanes = channels * obs
    eye = lax.broadcasted_iota(jnp.int32, (obs, obs), 0) == lax.broadcasted_iota(jnp.int32, (obs, obs), 1)
    owner = lax.broadcasted_iota(jnp.int32, (1, lanes), 1) // obs

    ft_ref[...] = turn_fading(fade_ref[...])

    def fade_lanes(step):
        out = fade_wide(ft_ref, step, 0, channels, slice(0, frames // LANES))
        for c in each[1:]:
            out = jnp.where(owner == c, fade_wide(ft_ref, step, c, channels, slice(0, frames // LANES)), out)
        return out

    weighted, closed, map_trans = [], [], []
    for c in each:
        column = jnp.sum(jnp.where(eye, weight_ref[c : c + 1, :], 0.0), axis=1, keepdims=True)
        observe = map_ref[c]
        weighted.append(observe * column)
        moved = exact(observe, trans_ref[c])
        map_trans.append(jnp.transpose(moved))
        closed.append(jnp.transpose(trans_ref[c]) - exact(map_trans[c], weighted[c]))

    load.wait()
    blocks_all = frames // LANES

    def turn(first, last):
        for b in range(first, last):
            piece = y_ref[:, :, b * LANES : (b + 1) * LANES].reshape(lanes, LANES)
            yt_ref[b] = jnp.transpose(regroup(piece, GROUP)).reshape(length, GROUP, lanes)

    stacks, power = list(weighted), list(closed)
    rounds = length.bit_length() - 1
    for level in range(rounds):
        turn(level * blocks_all // rounds, (level + 1) * blocks_all // rounds)
        for c in each:
            older = fast(rows_split(stacks[c]), pack(power[c]))
            stacks[c] = jnp.concatenate([stacks[c], older], axis=0)
            power[c] = exact(power[c], power[c])

    def spread(blocks):
        rows = []
        for c in each:
            parts = [blocks[c] if d == c else jnp.zeros_like(blocks[c]) for d in each]
            rows.append(jnp.concatenate(parts, axis=1))
        return jnp.concatenate(rows, axis=0)

    def inject_weight(blocks):
        high, low = halves(spread(blocks))
        return jnp.concatenate([high, high, low], axis=0)

    def obs_at(step):
        return yt_ref[:, step].reshape(count, lanes)

    turned = pltpu.make_async_copy(yt_ref, yt_hbm, yt_sem)
    turned.start()

    ends = jnp.zeros((count, channels * state), F32)
    decay = jnp.ones((count, lanes), F32)
    packed = []
    levels = count.bit_length() - 1
    every = max(length // levels, 1)
    for step in reversed(range(length)):
        age = length - 1 - step
        blocks = [stacks[c][age * obs : (age + 1) * obs] for c in each]
        ends = ends + inject(obs_at(step) * decay, inject_weight(blocks))
        decay = decay * fade_lanes(step)
        if len(packed) < levels and age % every == 0:
            packed.append([pack(power[c]) for c in each])
            power = [exact(power[c], power[c]) for c in each]

    row = lax.broadcasted_iota(jnp.int32, (count, state), 0)
    sums = [ends[:, c * state : (c + 1) * state] for c in each]
    factors = [jnp.broadcast_to(decay[:, c * obs : c * obs + 1], (count, state)) for c in each]
    while len(packed) < levels:
        packed.append([pack(power[c]) for c in each])
        power = [exact(power[c], power[c]) for c in each]
    for level in range(levels):
        reach = 1 << level
        for c in each:
            if reach < 8:
                before = rows_split(shifted(sums[c], reach, 0.0, row))
                sums[c] = sums[c] + factors[c] * fast(before, packed[level][c])
                factors[c] = factors[c] * shifted(factors[c], reach, 1.0, row)
            else:
                rest = count - reach
                moved = factors[c][reach:] * fast(rows_split(sums[c][:rest]), packed[level][c])
                sums[c] = jnp.concatenate([sums[c][:reach], sums[c][reach:] + moved], axis=0)
                joined = factors[c][reach:] * factors[c][:rest]
                factors[c] = jnp.concatenate([factors[c][:reach], joined], axis=0)

    last = [part[c][count - 1 : count, :] for part in (sums, factors) for c in each]
    end_src[...] = jnp.concatenate(last + [jnp.zeros((8 - len(last), state), F32)], axis=0)
    pl.semaphore_wait(barrier, len(peers))
    sends = swap(end_src, end_got, end_send, end_recv, peers)

    sums = [shifted(sums[c], 1, 0.0, row) for c in each]
    factors = [shifted(factors[c], 1, 1.0, row) for c in each]
    for c in each:
        step_ref[c] = pack(closed[c])
    pred_ref[...] = jnp.concatenate(halves(spread(map_trans)), axis=1)
    now_ref[...] = inject_weight(weighted)
    section = [pack(power[c]) for c in each]

    for copy in sends:
        copy.wait()

    enter = [jnp.zeros((8, state), F32) for c in each]
    for j in range(tm - 1):
        slot = jnp.maximum(lax.rem(my_tm - j + tm, tm) - 1, 0)
        got = end_got[slot]
        for c in each:
            value = jnp.broadcast_to(got[c : c + 1, :], (8, state))
            if j > 0:
                value = value + got[channels + c : channels + c + 1, :] * fast(
                    rows_split(enter[c]), section[c]
                )
            enter[c] = jnp.where(j < my_tm, value, enter[c])

    small = lax.broadcasted_iota(jnp.int32, (8, state), 0)
    for c in each:
        carried = enter[c]
        for level, weights in enumerate(packed):
            further = fast(rows_split(carried), weights[c])
            size = 1 << level
            if size < 8:
                carried = jnp.where(small < size, carried, pltpu.roll(further, size, 0))
            else:
                carried = jnp.concatenate([carried, further], axis=0)
        x_ref[c] = sums[c] + factors[c] * carried[:count]
    turned.wait()


def step_kernel(
    yt_hbm, ft_ref, x_ref, step_ref, pred_ref, now_ref, prec_ref, states_hbm, nis_ref,
    yt_ref, xt_ref, out_ref, in_sem, out_sem,
):
    channels, count, state = x_ref.shape
    lanes = yt_ref.shape[3]
    frames = count * CHUNK
    each = range(channels)
    loads = []
    for step in range(CHUNK):
        load = pltpu.make_async_copy(yt_hbm.at[:, step], yt_ref.at[:, step], in_sem.at[step])
        load.start()
        loads.append(load)
    prec = jnp.concatenate([prec_ref[c : c + 1, :] for c in each], axis=1)
    owner = lax.broadcasted_iota(jnp.int32, (1, lanes), 1) // (lanes // channels)
    batches = nis_ref.shape[1]
    blocks = frames // LANES // PARTS
    rows = count // PARTS
    per = []
    stores = []

    def finish(b):
        for c in each:
            piece = jnp.transpose(xt_ref[c, b].reshape(LANES, state))
            out_ref[c, :, b * LANES : (b + 1) * LANES] = regroup(piece, CHUNK)

    def send(part):
        for c in each:
            span = pl.ds(part * blocks * LANES // SPANS, blocks * LANES // SPANS)
            store = pltpu.make_async_copy(
                out_ref.at[c, :, span], states_hbm.at[c, :, span], out_sem.at[c, part]
            )
            store.start()
            stores.append(store)

    waited = 0
    for part in range(PARTS):
        norms = jnp.zeros((rows, lanes), F32)
        x = [x_ref[c, part * rows : (part + 1) * rows] for c in each]
        done = 0
        for step in range(CHUNK):
            if part == 0 and step == waited:
                more = min(CHUNK, max(2, 3 * waited))
                for load in loads[waited:more]:
                    load.wait()
                waited = more
            span = slice(part * blocks, (part + 1) * blocks)
            observed = yt_ref[span, step].reshape(rows, lanes)
            wide = [fade_wide(ft_ref, step, c, channels, span) for c in each]
            mixed = wide[0]
            for c in each[1:]:
                mixed = jnp.where(owner == c, wide[c], mixed)
            added = inject(observed, now_ref[...])
            parts = [halves(x[c]) for c in each]
            rounded = jnp.concatenate([part_[0] for part_ in parts], axis=1)
            innovation = observed - mixed * fast(rounded, pred_ref[...])
            norms = norms + prec * innovation * innovation
            for c in each:
                moved = fast(jnp.concatenate(parts[c], axis=1), step_ref[c])
                x[c] = wide[c] * moved + added[:, c * state : (c + 1) * state]
                xt_ref[c, span, step] = x[c].reshape(blocks, GROUP, state)
            if part > 0:
                ready = blocks * (step + 1) // CHUNK
                for b in range(done, ready):
                    finish((part - 1) * blocks + b)
                done = ready
        if part > 0:
            for k in range(SPANS):
                send((part - 1) * SPANS + k)
        per.append(jnp.sum(norms.reshape(batches // PARTS, rows * PARTS // batches, lanes), axis=1))

    per_batch = jnp.concatenate(per, axis=0)
    nis_ref[...] = dot(jnp.ones((8, lanes), F32), per_batch, ((1,), (1,)))
    for k in range(SPANS):
        for b in range(k * blocks // SPANS, (k + 1) * blocks // SPANS):
            finish((PARTS - 1) * blocks + b)
        send((PARTS - 1) * SPANS + k)
    for store in stores:
        store.wait()


def norm_kernel(chan, divisor, mine_ref, nis_ref, got, send_sem, recv_sem):
    barrier, peers = greet("chan", chan, lax.axis_index("chan"))
    pl.semaphore_wait(barrier, len(peers))
    sends = swap(mine_ref, got, send_sem, recv_sem, peers)
    total = mine_ref[0:1, :]
    for d, copy in enumerate(sends):
        copy.wait()
        total = total + got[d, 0:1, :]
    nis_ref[...] = total / divisor


def per_device(tm, chan, observations, transition, obs_map, measured_weighting, obs_precision, fading):
    channels, obs, frames = observations.shape
    state = transition.shape[1]
    batches = frames // MB_FRAMES
    count = frames // CHUNK
    lanes = channels * obs
    vmem = pl.BlockSpec(memory_space=pltpu.VMEM)
    hbm = pl.BlockSpec(memory_space=pl.ANY)
    dma = pltpu.SemaphoreType.DMA
    shape = jax.ShapeDtypeStruct
    limit = 56 * 1024 * 1024
    turned = (frames // LANES, CHUNK, GROUP, lanes)
    handed = pl.pallas_call(
        functools.partial(enter_kernel, tm),
        out_shape=(
            shape(turned, F32),
            shape((LANES, LANES), F32),
            shape((channels, count, state), F32),
            shape((channels, 2 * state, 2 * state), BF16),
            shape((channels * state, 2 * lanes), BF16),
            shape((3 * lanes, channels * state), BF16),
        ),
        in_specs=[hbm] + [vmem] * 4,
        out_specs=(hbm,) + (vmem,) * 5,
        scratch_shapes=[
            pltpu.VMEM((channels, obs, frames), F32),
            pltpu.VMEM(turned, F32),
            pltpu.VMEM((8, state), F32),
            pltpu.VMEM((max(tm - 1, 1), 8, state), F32),
            dma(()),
            dma(()),
            dma((max(tm - 1, 1),)),
            dma((max(tm - 1, 1),)),
        ],
        compiler_params=pltpu.CompilerParams(
            collective_id=0, has_side_effects=True, vmem_limit_bytes=limit
        ),
        name="enter",
    )(observations, transition, obs_map, measured_weighting, fading)
    states, mine = pl.pallas_call(
        step_kernel,
        out_shape=(shape((channels, state, frames), F32), shape((8, batches), F32)),
        in_specs=[hbm] + [vmem] * 6,
        out_specs=(hbm, vmem),
        scratch_shapes=[
            pltpu.VMEM(turned, F32),
            pltpu.VMEM((channels, frames // LANES, CHUNK, GROUP, state), F32),
            pltpu.VMEM((channels, state, frames), F32),
            dma((CHUNK,)),
            dma((channels, PARTS * SPANS)),
        ],
        compiler_params=pltpu.CompilerParams(vmem_limit_bytes=limit),
        name="steps",
    )(*handed, obs_precision)
    nis = pl.pallas_call(
        functools.partial(norm_kernel, chan, channels * chan * MB_FRAMES * obs),
        out_shape=shape((1, batches), F32),
        in_specs=[vmem],
        out_specs=vmem,
        scratch_shapes=[
            pltpu.VMEM((max(chan - 1, 1), 8, batches), F32),
            dma((max(chan - 1, 1),)),
            dma((max(chan - 1, 1),)),
        ],
        compiler_params=pltpu.CompilerParams(collective_id=1, has_side_effects=True),
        name="norms",
    )(mine)
    return states, nis.reshape(batches)


def solution(mesh):
    in_specs = (
        P("chan", None, "tm"),
        P("chan", None, None),
        P("chan", None, None),
        P("chan", None),
        P("chan", None),
        P("chan", "tm"),
    )
    out_specs = (P("chan", None, "tm"), P("tm"))
    body = functools.partial(per_device, mesh.shape["tm"], mesh.shape["chan"])
    return jax.shard_map(body, mesh=mesh, in_specs=in_specs, out_specs=out_specs, check_vma=False)
```

```python
import functools

import jax
import jax.numpy as jnp
from jax import lax
from jax.experimental import pallas as pl
from jax.experimental.pallas import tpu as pltpu
from jax.sharding import PartitionSpec as P

MB_FRAMES = 128
LANES = 128
GROUP = 8
CHUNK = LANES // GROUP
HIGHEST = lax.Precision.HIGHEST
F32 = jnp.float32
BF16 = jnp.bfloat16


def dot(a, b, dims=((1,), (0,)), precision=HIGHEST):
    return lax.dot_general(a, b, (dims, ((), ())), precision=precision, preferred_element_type=F32)


def halves(x):
    high = x.astype(BF16)
    low = (x - high.astype(F32)).astype(BF16)
    return high, low


def thirds(x):
    high = x.astype(BF16)
    rest = x - high.astype(F32)
    mid = rest.astype(BF16)
    return high, mid, (rest - mid.astype(F32)).astype(BF16)


def exact(a, b):
    a_high, a_mid, a_low = thirds(a)
    b_high, b_mid, b_low = thirds(b)
    top = jnp.concatenate([b_high, b_mid], axis=1)
    wide = dot(
        jnp.concatenate([a_high, a_mid], axis=1),
        jnp.concatenate([top, top], axis=0),
        precision=None,
    )
    tail = dot(
        jnp.concatenate([a_high, a_low], axis=1),
        jnp.concatenate([b_low, b_high], axis=0),
        precision=None,
    )
    half = b.shape[1]
    return wide[:, :half] + (wide[:, half:] + tail)


def rows_split(x):
    return jnp.concatenate(halves(x), axis=1)


def pack(weight):
    high, low = halves(weight)
    top = jnp.concatenate([high, low], axis=1)
    return jnp.concatenate([top, top], axis=0)


def fast(split, packed):
    both = dot(split, packed, precision=None)
    half = both.shape[1] // 2
    return both[:, :half] + both[:, half:]


def regroup(x, groups):
    place = lax.broadcasted_iota(jnp.int32, x.shape, 1)
    source = (place % groups) * (LANES // groups) + place // groups
    return jnp.take_along_axis(x, source, axis=1, mode="promise_in_bounds")


def shifted(x, reach, fill, row):
    return jnp.where(row >= reach, pltpu.roll(x, reach, 0), fill)


def kernel(
    tm, chan, y_hbm, trans_ref, map_ref, weight_ref, prec_ref, fade_ref, states_hbm, nis_ref,
    y_ref, yt_ref, ft_ref, xt_ref, out_ref, end_src, end_got, nis_src, nis_got,
    in_sem, out_sem, end_send, end_recv, nis_send, nis_recv,
):
    channels, obs, frames = y_ref.shape
    state = trans_ref.shape[1]
    length = CHUNK
    count = frames // length
    my_tm, my_chan = lax.axis_index("tm"), lax.axis_index("chan")

    def peer(axis, size, mine, offset):
        return {axis: lax.rem(mine + offset, size)}

    peers = [peer("tm", tm, my_tm, d) for d in range(1, tm)]
    peers += [peer("chan", chan, my_chan, d) for d in range(1, chan)]
    barrier = pltpu.get_barrier_semaphore()
    for target in peers:
        pl.semaphore_signal(barrier, inc=1, device_id=target, device_id_type=pl.DeviceIdType.MESH)
    load = pltpu.make_async_copy(y_hbm, y_ref, in_sem)
    load.start()

    each = range(channels)
    lanes = channels * obs
    eye = lax.broadcasted_iota(jnp.int32, (obs, obs), 0) == lax.broadcasted_iota(jnp.int32, (obs, obs), 1)
    owner = lax.broadcasted_iota(jnp.int32, (1, lanes), 1) // obs

    fade = jnp.concatenate([fade_ref[...]] * (8 // channels), axis=0)
    for b in range(frames // LANES):
        piece = regroup(fade[:, b * LANES : (b + 1) * LANES], GROUP)
        ft_ref[b] = jnp.transpose(piece).reshape(length, GROUP, 8)

    def fade_at(step):
        return ft_ref[:, step].reshape(count, 8)

    def fade_lanes(columns):
        out = jnp.broadcast_to(columns[:, 0:1], (count, lanes))
        for c in each[1:]:
            out = jnp.where(owner == c, columns[:, c : c + 1], out)
        return out

    weighted, closed, map_trans = [], [], []
    for c in each:
        column = jnp.sum(jnp.where(eye, weight_ref[c : c + 1, :], 0.0), axis=1, keepdims=True)
        observe = map_ref[c]
        weighted.append(observe * column)
        moved = exact(observe, trans_ref[c])
        map_trans.append(jnp.transpose(moved))
        closed.append(jnp.transpose(trans_ref[c]) - exact(map_trans[c], weighted[c]))

    load.wait()
    blocks_all = frames // LANES

    def turn(first, last):
        for b in range(first, last):
            piece = y_ref[:, :, b * LANES : (b + 1) * LANES].reshape(lanes, LANES)
            yt_ref[b] = jnp.transpose(regroup(piece, GROUP)).reshape(length, GROUP, lanes)

    stacks, power = list(weighted), list(closed)
    rounds = length.bit_length() - 1
    for level in range(rounds):
        turn(level * blocks_all // rounds, (level + 1) * blocks_all // rounds)
        for c in each:
            older = fast(rows_split(stacks[c]), pack(power[c]))
            stacks[c] = jnp.concatenate([stacks[c], older], axis=0)
            power[c] = exact(power[c], power[c])

    def spread(blocks):
        rows = []
        for c in each:
            parts = [blocks[c] if d == c else jnp.zeros_like(blocks[c]) for d in each]
            rows.append(jnp.concatenate(parts, axis=1))
        return jnp.concatenate(rows, axis=0)

    def inject_weight(blocks):
        high, low = halves(spread(blocks))
        return jnp.concatenate([high, high, low], axis=0)

    def inject(values, weight):
        high, low = halves(values)
        return dot(jnp.concatenate([high, low, high], axis=1), weight, precision=None)

    def obs_at(step):
        return yt_ref[:, step].reshape(count, lanes)

    ends = jnp.zeros((count, channels * state), F32)
    decay = jnp.ones((count, lanes), F32)
    packed = []
    levels = count.bit_length() - 1
    every = max(length // levels, 1)
    for step in reversed(range(length)):
        age = length - 1 - step
        blocks = [stacks[c][age * obs : (age + 1) * obs] for c in each]
        ends = ends + inject(obs_at(step) * decay, inject_weight(blocks))
        decay = decay * fade_lanes(fade_at(step))
        if len(packed) < levels and age % every == 0:
            packed.append([pack(power[c]) for c in each])
            power = [exact(power[c], power[c]) for c in each]

    row = lax.broadcasted_iota(jnp.int32, (count, state), 0)
    sums = [ends[:, c * state : (c + 1) * state] for c in each]
    factors = [jnp.broadcast_to(decay[:, c * obs : c * obs + 1], (count, state)) for c in each]
    while len(packed) < levels:
        packed.append([pack(power[c]) for c in each])
        power = [exact(power[c], power[c]) for c in each]
    for level in range(levels):
        reach = 1 << level
        for c in each:
            if reach < GROUP:
                before = rows_split(shifted(sums[c], reach, 0.0, row))
                sums[c] = sums[c] + factors[c] * fast(before, packed[level][c])
                factors[c] = factors[c] * shifted(factors[c], reach, 1.0, row)
            else:
                rest = count - reach
                moved = factors[c][reach:] * fast(rows_split(sums[c][:rest]), packed[level][c])
                sums[c] = jnp.concatenate([sums[c][:reach], sums[c][reach:] + moved], axis=0)
                joined = factors[c][reach:] * factors[c][:rest]
                factors[c] = jnp.concatenate([factors[c][:reach], joined], axis=0)

    last = [part[c][count - 1 : count, :] for part in (sums, factors) for c in each]
    end_src[...] = jnp.concatenate(last + [jnp.zeros((8 - len(last), state), F32)], axis=0)
    pl.semaphore_wait(barrier, len(peers))
    sends = []
    for d in range(1, tm):
        copy = pltpu.make_async_remote_copy(
            src_ref=end_src, dst_ref=end_got.at[d - 1], send_sem=end_send.at[d - 1],
            recv_sem=end_recv.at[d - 1], device_id=peers[d - 1], device_id_type=pl.DeviceIdType.MESH,
        )
        copy.start()
        sends.append(copy)

    sums = [shifted(sums[c], 1, 0.0, row) for c in each]
    factors = [shifted(factors[c], 1, 1.0, row) for c in each]
    step_weight = [pack(closed[c]) for c in each]
    pred_weight = jnp.concatenate(halves(spread(map_trans)), axis=1)
    now_weight = inject_weight(weighted)
    section = [pack(power[c]) for c in each]

    for copy in sends:
        copy.wait()

    enter = [jnp.zeros((8, state), F32) for c in each]
    for j in range(tm - 1):
        slot = jnp.maximum(lax.rem(my_tm - j + tm, tm) - 1, 0)
        got = end_got[slot]
        for c in each:
            value = jnp.broadcast_to(got[c : c + 1, :], (8, state))
            if j > 0:
                value = value + got[channels + c : channels + c + 1, :] * fast(
                    rows_split(enter[c]), section[c]
                )
            enter[c] = jnp.where(j < my_tm, value, enter[c])

    x = []
    small = lax.broadcasted_iota(jnp.int32, (8, state), 0)
    for c in each:
        carried = enter[c]
        for level, weights in enumerate(packed):
            further = fast(rows_split(carried), weights[c])
            size = 1 << level
            if size < 8:
                carried = jnp.where(small < size, carried, pltpu.roll(further, size, 0))
            else:
                carried = jnp.concatenate([carried, further], axis=0)
        x.append(sums[c] + factors[c] * carried[:count])

    prec = jnp.concatenate([prec_ref[c : c + 1, :] for c in each], axis=1)
    norms = jnp.zeros((count, lanes), F32)
    for step in range(length):
        observed = obs_at(step)
        columns = fade_at(step)
        added = inject(observed, now_weight)
        wide = [jnp.broadcast_to(columns[:, c : c + 1], (count, LANES)) for c in each]
        mixed = wide[0]
        for c in each[1:]:
            mixed = jnp.where(owner == c, wide[c], mixed)
        parts = [halves(x[c]) for c in each]
        rounded = jnp.concatenate([part[0] for part in parts], axis=1)
        innovation = observed - mixed * fast(rounded, pred_weight)
        for c in each:
            moved = fast(jnp.concatenate(parts[c], axis=1), step_weight[c])
            x[c] = wide[c] * moved + added[:, c * state : (c + 1) * state]
            xt_ref[c, :, step] = x[c].reshape(blocks_all, GROUP, state)
        norms = norms + prec * innovation * innovation

    batches = nis_ref.shape[1]
    per_batch = jnp.sum(norms.reshape(batches, count // batches, lanes), axis=1)
    nis_src[...] = dot(jnp.ones((8, lanes), F32), per_batch, ((1,), (1,)))
    sends = []
    for d in range(1, chan):
        copy = pltpu.make_async_remote_copy(
            src_ref=nis_src, dst_ref=nis_got.at[d - 1], send_sem=nis_send.at[d - 1],
            recv_sem=nis_recv.at[d - 1], device_id=peers[tm - 1 + d - 1],
            device_id_type=pl.DeviceIdType.MESH,
        )
        copy.start()
        sends.append(copy)

    stores = []
    block = frames // out_sem.shape[1]
    for c in each:
        for index in range(out_sem.shape[1]):
            for start in range(index * block, (index + 1) * block, LANES):
                piece = jnp.transpose(xt_ref[c, start // LANES].reshape(LANES, state))
                out_ref[c, :, start : start + LANES] = regroup(piece, CHUNK)
            span = pl.ds(index * block, block)
            store = pltpu.make_async_copy(
                out_ref.at[c, :, span], states_hbm.at[c, :, span], out_sem.at[c, index]
            )
            store.start()
            stores.append(store)

    for copy in sends:
        copy.wait()
    total = nis_src[0:1, :]
    for d in range(1, chan):
        total = total + nis_got[d - 1, 0:1, :]
    nis_ref[...] = total / (channels * chan * MB_FRAMES * obs)
    for store in stores:
        store.wait()


def per_device(tm, chan, observations, transition, obs_map, measured_weighting, obs_precision, fading):
    channels, obs, frames = observations.shape
    state = transition.shape[1]
    batches = frames // MB_FRAMES
    lanes = channels * obs
    vmem = pl.BlockSpec(memory_space=pltpu.VMEM)
    hbm = pl.BlockSpec(memory_space=pl.ANY)
    dma = pltpu.SemaphoreType.DMA
    grouped = (channels, frames // LANES, CHUNK, GROUP, state)
    states, nis = pl.pallas_call(
        functools.partial(kernel, tm, chan),
        out_shape=(
            jax.ShapeDtypeStruct((channels, state, frames), F32),
            jax.ShapeDtypeStruct((1, batches), F32),
        ),
        in_specs=[hbm] + [vmem] * 5,
        out_specs=(hbm, vmem),
        scratch_shapes=[
            pltpu.VMEM((channels, obs, frames), F32),
            pltpu.VMEM((frames // LANES, CHUNK, GROUP, lanes), F32),
            pltpu.VMEM((frames // LANES, CHUNK, GROUP, 8), F32),
            pltpu.VMEM(grouped, F32),
            pltpu.VMEM((channels, state, frames), F32),
            pltpu.VMEM((8, state), F32),
            pltpu.VMEM((max(tm - 1, 1), 8, state), F32),
            pltpu.VMEM((8, batches), F32),
            pltpu.VMEM((max(chan - 1, 1), 8, batches), F32),
            dma(()),
            dma((channels, 2)),
            dma((max(tm - 1, 1),)),
            dma((max(tm - 1, 1),)),
            dma((max(chan - 1, 1),)),
            dma((max(chan - 1, 1),)),
        ],
        compiler_params=pltpu.CompilerParams(
            collective_id=0, has_side_effects=True, vmem_limit_bytes=56 * 1024 * 1024
        ),
        name="filter",
    )(observations, transition, obs_map, measured_weighting, obs_precision, fading)
    return states, nis.reshape(batches)


def solution(mesh):
    in_specs = (
        P("chan", None, "tm"),
        P("chan", None, None),
        P("chan", None, None),
        P("chan", None),
        P("chan", None),
        P("chan", "tm"),
    )
    out_specs = (P("chan", None, "tm"), P("tm"))
    body = functools.partial(per_device, mesh.shape["tm"], mesh.shape["chan"])
    return jax.shard_map(body, mesh=mesh, in_specs=in_specs, out_specs=out_specs, check_vma=False)
```
